32 devices in a mesh: row: 4 (over y, core), col: 4 (over z), rep: 2 (over x).
Axes of the slice: x: 2, y: 2, z: 4, core: 2. Of those that a mesh axis runs over, the one named last changes fastest.
Arguments:
- features: bfloat16 [2, 128, 128, 512], P('rep', 'row', 'col'), may hold values from -6 to 6
- cotangent: bfloat16 [2, 128, 128, 512], P('rep', 'row', 'col'), may hold values from -6 to 6
- depthwise_filters: float32 [2, 7, 7, 512], replicated, may hold values from -0.875 to 0.875
- depthwise_bias_vector: float32 [2, 512], replicated, may hold values from -1.5 to 1.5
- layernorm_gain: float32 [2, 512], replicated, may hold values from 0.5 to 1.5
- layernorm_shift: float32 [2, 512], replicated, may hold values from -1.5 to 1.5
- inner_frozen_weight: bfloat16 [2, 512, 2048], replicated, may hold values from -0.25 to 0.25
- outer_frozen_weight: bfloat16 [2, 2048, 512], replicated, may hold values from -0.125 to 0.125
- inner_down_factor: bfloat16 [2, 512, 16], replicated, may hold values from -0.25 to 0.25
- inner_up_factor: bfloat16 [2, 16, 2048], replicated, may hold values from -0.75 to 0.75
- outer_down_factor: bfloat16 [2, 2048, 16], replicated, may hold values from -0.125 to 0.125
- outer_up_factor: bfloat16 [2, 16, 512], replicated, may hold values from -0.75 to 0.75
- branch_channel_scale: float32 [2, 512], replicated, may hold values from 0.2 to 1
Outputs:
- features_out: bfloat16 [2, 128, 128, 512], P('rep', 'row', 'col')
- step_a_in: float32 [2, 512, 16], replicated
- step_b_in: float32 [2, 16, 2048], replicated
- step_a_out: float32 [2, 2048, 16], replicated
- step_b_out: float32 [2, 16, 512], replicated
The draws below stay inside these ranges and needn't reach their ends.
All inputs are finite; a program needn't handle non-finite values.
Results may differ from the reference program's by a relative error of at most 0.013.
Values may be sent and summed in bfloat16 or wider, within the bound.
A program may use at most 128 MiB of HBM per device.

```python
import math
import jax
import jax.numpy as jnp
from jax import lax

CHANNEL_COUNT = 512
HIDDEN_UNITS = 2048
ADAPTER_RANK = 16
BLOCK_COUNT = 2
H = 128
W = 128
IMAGES = 2


def levels(stream_key, extent, pieces, smallest, top_value):
    def one(axis_at, parts):
        draws = jax.random.uniform(jax.random.fold_in(jax.random.fold_in(stream_key, 6), axis_at), (parts,), jnp.float32, smallest / len(pieces), top_value / len(pieces))
        return jnp.repeat(jnp.exp(draws), extent[axis_at] // parts).reshape((-1,) + (1,) * (len(extent) - axis_at - 1))

    loudness = one(*pieces[0])
    for cut in pieces[1:]:
        loudness = loudness * one(*cut)
    return loudness


def scatter_about(key, shape, width, limit, split=(), held_as=jnp.bfloat16):
    entries = width * jax.random.normal(key, shape, jnp.float32)
    if split:
        entries = entries * levels(key, shape, split, -0.22, 0.18)
    return jnp.clip(entries, -limit, limit).astype(held_as)


def setup_inputs(seed: int = 0) -> dict:
    seeds = jax.random.split(jax.random.key(seed), 14)
    features = scatter_about(seeds[0], (IMAGES, H, W, CHANNEL_COUNT), 1.0, 6.0, ((0, 2), (1, 4), (2, 4)))
    cotangent = scatter_about(seeds[1], (IMAGES, H, W, CHANNEL_COUNT), 1.0, 6.0, ((0, 2), (1, 4), (2, 4)))
    depthwise_filters = scatter_about(seeds[2], (BLOCK_COUNT, 7, 7, CHANNEL_COUNT), 49 ** -0.5, 0.875, (), jnp.float32)
    depthwise_bias_vector = scatter_about(seeds[3], (BLOCK_COUNT, CHANNEL_COUNT), 0.3, 1.5, (), jnp.float32)
    layernorm_gain = jnp.clip(1.0 + 0.1 * jax.random.normal(seeds[4], (BLOCK_COUNT, CHANNEL_COUNT), jnp.float32), 0.5, 1.5)
    layernorm_shift = scatter_about(seeds[5], (BLOCK_COUNT, CHANNEL_COUNT), 0.3, 1.5, (), jnp.float32)
    inner_frozen_weight = scatter_about(seeds[6], (BLOCK_COUNT, CHANNEL_COUNT, HIDDEN_UNITS), CHANNEL_COUNT ** -0.5, 0.25)
    outer_frozen_weight = scatter_about(seeds[7], (BLOCK_COUNT, HIDDEN_UNITS, CHANNEL_COUNT), HIDDEN_UNITS ** -0.5, 0.125)
    inner_down_factor = scatter_about(seeds[8], (BLOCK_COUNT, CHANNEL_COUNT, ADAPTER_RANK), CHANNEL_COUNT ** -0.5, 0.25)
    inner_up_factor = scatter_about(seeds[9], (BLOCK_COUNT, ADAPTER_RANK, HIDDEN_UNITS), (4 * ADAPTER_RANK) ** -0.5, 0.75)
    outer_down_factor = scatter_about(seeds[10], (BLOCK_COUNT, HIDDEN_UNITS, ADAPTER_RANK), HIDDEN_UNITS ** -0.5, 0.125)
    outer_up_factor = scatter_about(seeds[11], (BLOCK_COUNT, ADAPTER_RANK, CHANNEL_COUNT), (4 * ADAPTER_RANK) ** -0.5, 0.75)
    branch_channel_scale = jnp.clip(jnp.exp(jax.random.uniform(seeds[12], (BLOCK_COUNT, CHANNEL_COUNT), jnp.float32, math.log(0.2), math.log(1.0))), 0.2, 1.0)
    return {"features": features, "cotangent": cotangent, "depthwise_filters": depthwise_filters, "depthwise_bias_vector": depthwise_bias_vector, "layernorm_gain": layernorm_gain, "layernorm_shift": layernorm_shift, "inner_frozen_weight": inner_frozen_weight, "outer_frozen_weight": outer_frozen_weight, "inner_down_factor": inner_down_factor, "inner_up_factor": inner_up_factor, "outer_down_factor": outer_down_factor, "outer_up_factor": outer_up_factor, "branch_channel_scale": branch_channel_scale}


adapter_scale = 2.0
norm_eps = 1e-06
step_eps = 1e-06
gelu_coef = 0.7978845608

def depthwise(padded, kernel, bias, rows, cols):
    total = jnp.zeros(padded.shape[:1] + (rows, cols, padded.shape[3]), jnp.float32) + bias
    for first in range(7):
        for second in range(7):
            total = total + padded[:, first:first + rows, second:second + cols, :].astype(jnp.float32) * kernel[first, second]
    return total

def gelu_parts(preactivation):
    inner = gelu_coef * (preactivation + 0.044715 * preactivation * preactivation * preactivation)
    tangent = jnp.tanh(inner)
    value = 0.5 * preactivation * (1.0 + tangent)
    activation_slope = 0.5 * (1.0 + tangent) + 0.5 * preactivation * (1.0 - tangent * tangent) * gelu_coef * (1.0 + 3.0 * 0.044715 * preactivation * preactivation)
    return (value, activation_slope)

def multiply_matrices(left, right):
    return jnp.dot(left, right, preferred_element_type=jnp.float32)

def pointwise_forward(flat_block, weights):
    inner_frozen, outer_frozen, inner_down, inner_up, outer_down, outer_up = weights
    inner_middle = multiply_matrices(flat_block, inner_down).astype(jnp.bfloat16)
    preactivation = multiply_matrices(flat_block, inner_frozen) + adapter_scale * multiply_matrices(inner_middle, inner_up)
    value, activation_slope = gelu_parts(preactivation)
    hidden_activation = value.astype(jnp.bfloat16)
    outer_middle = multiply_matrices(hidden_activation, outer_down).astype(jnp.bfloat16)
    branch = multiply_matrices(hidden_activation, outer_frozen) + adapter_scale * multiply_matrices(outer_middle, outer_up)
    return (branch, inner_middle, activation_slope, hidden_activation, outer_middle)

def pointwise_backward(flat_block, output_gradient, weights):
    inner_frozen, outer_frozen, inner_down, inner_up, outer_down, outer_up = weights
    unused_branch, inner_middle, activation_slope, hidden_activation, outer_middle = pointwise_forward(flat_block, weights)
    outer_up_gradient = adapter_scale * multiply_matrices(outer_middle.T, output_gradient)
    outer_mid_gradient = (adapter_scale * multiply_matrices(output_gradient, outer_up.T)).astype(jnp.bfloat16)
    grad_a_out = multiply_matrices(hidden_activation.T, outer_mid_gradient)
    hidden_gradient = multiply_matrices(output_gradient, outer_frozen.T) + multiply_matrices(outer_mid_gradient, outer_down.T)
    preact_gradient = (hidden_gradient * activation_slope).astype(jnp.bfloat16)
    inner_up_gradient = adapter_scale * multiply_matrices(inner_middle.T, preact_gradient)
    inner_mid_gradient = (adapter_scale * multiply_matrices(preact_gradient, inner_up.T)).astype(jnp.bfloat16)
    grad_a_in = multiply_matrices(flat_block.T, inner_mid_gradient)
    normed_gradient = multiply_matrices(preact_gradient, inner_frozen.T) + multiply_matrices(inner_mid_gradient, inner_down.T)
    return (normed_gradient, (grad_a_in, inner_up_gradient, grad_a_out, outer_up_gradient))

def picture_forward_backward(image_tensor, cotangent, depthwise_filters, depthwise_bias_vector, layernorm_gain, layernorm_shift, inner_frozen_weight, outer_frozen_weight, inner_down_factor, inner_up_factor, outer_down_factor, outer_up_factor, branch_channel_scale):
    rows, cols, chans = (image_tensor.shape[1], image_tensor.shape[2], image_tensor.shape[3])
    pixel_total = rows * cols
    group_rows = math.gcd(pixel_total, 2048)
    group_count = pixel_total // group_rows
    current = image_tensor
    saved_activations = []
    for block_layer in range(BLOCK_COUNT):
        weights = (inner_frozen_weight[block_layer], outer_frozen_weight[block_layer], inner_down_factor[block_layer], inner_up_factor[block_layer], outer_down_factor[block_layer], outer_up_factor[block_layer])
        padded = jnp.pad(current, ((0, 0), (3, 3), (3, 3), (0, 0)))
        conv = depthwise(padded, depthwise_filters[block_layer], depthwise_bias_vector[block_layer], rows, cols)
        channel_mean = lax.optimization_barrier(jnp.mean(conv, -1, keepdims=True))
        centered_input = conv - channel_mean
        inverse_deviation = lax.rsqrt(lax.optimization_barrier(jnp.mean(centered_input * centered_input, -1, keepdims=True)) + norm_eps)
        standardized_input = centered_input * inverse_deviation
        normed_features = (standardized_input * layernorm_gain[block_layer] + layernorm_shift[block_layer]).astype(jnp.bfloat16)
        grouped_pixels = normed_features.reshape(group_count, group_rows, chans)
        residual_branch = lax.map(lambda flat_block: pointwise_forward(flat_block, weights)[0], grouped_pixels)
        current = (current.astype(jnp.float32) + branch_channel_scale[block_layer] * residual_branch.reshape(current.shape)).astype(jnp.bfloat16)
        saved_activations.append((grouped_pixels, standardized_input, inverse_deviation))
    grad_x = cotangent.astype(jnp.float32)
    adapter_gradients = [None] * BLOCK_COUNT
    for block_layer in range(BLOCK_COUNT - 1, -1, -1):
        weights = (inner_frozen_weight[block_layer], outer_frozen_weight[block_layer], inner_down_factor[block_layer], inner_up_factor[block_layer], outer_down_factor[block_layer], outer_up_factor[block_layer])
        grouped_pixels, standardized_input, inverse_deviation = saved_activations[block_layer]
        output_gradient = (grad_x * branch_channel_scale[block_layer]).astype(jnp.bfloat16).reshape(group_count, group_rows, chans)
        initial = (jnp.zeros(inner_down_factor.shape[1:], jnp.float32), jnp.zeros(inner_up_factor.shape[1:], jnp.float32), jnp.zeros(outer_down_factor.shape[1:], jnp.float32), jnp.zeros(outer_up_factor.shape[1:], jnp.float32))

        def accumulate(carry, inputs):
            normed_gradient, gradients = pointwise_backward(inputs[0], inputs[1], weights)
            return (tuple((carry[which] + gradients[which] for which in range(4))), normed_gradient)
        totals, normed_gradient = lax.scan(accumulate, initial, (grouped_pixels, output_gradient))
        adapter_gradients[block_layer] = totals
        if block_layer > 0:
            scaled_branch = normed_gradient.reshape(standardized_input.shape) * layernorm_gain[block_layer]
            conv_gradient = inverse_deviation * (scaled_branch - lax.optimization_barrier(jnp.mean(scaled_branch, -1, keepdims=True)) - standardized_input * lax.optimization_barrier(jnp.mean(scaled_branch * standardized_input, -1, keepdims=True)))
            conv_gradient = conv_gradient.astype(jnp.bfloat16)
            padded = jnp.pad(conv_gradient, ((0, 0), (3, 3), (3, 3), (0, 0)))
            flipped = depthwise_filters[block_layer][::-1, ::-1, :]
            grad_x = grad_x + depthwise(padded, flipped, jnp.zeros((chans,), jnp.float32), rows, cols)
    return (current, adapter_gradients)

def normalize(stacked):
    channel_mean = lax.optimization_barrier(jnp.mean(stacked * stacked, axis=(1, 2), keepdims=True))
    return stacked * lax.rsqrt(channel_mean + step_eps)

def reference(features, cotangent, depthwise_filters, depthwise_bias_vector, layernorm_gain, layernorm_shift, inner_frozen_weight, outer_frozen_weight, inner_down_factor, inner_up_factor, outer_down_factor, outer_up_factor, branch_channel_scale):
    outputs = []
    totals = None
    for picture_index in range(IMAGES):
        step_result, adapter_gradients = picture_forward_backward(features[picture_index:picture_index + 1], cotangent[picture_index:picture_index + 1], depthwise_filters, depthwise_bias_vector, layernorm_gain, layernorm_shift, inner_frozen_weight, outer_frozen_weight, inner_down_factor, inner_up_factor, outer_down_factor, outer_up_factor, branch_channel_scale)
        outputs.append(step_result)
        stacked = [jnp.stack([adapter_gradients[block_layer][which] for block_layer in range(BLOCK_COUNT)]) for which in range(4)]
        totals = stacked if totals is None else [totals[which] + stacked[which] for which in range(4)]
    features_out = jnp.concatenate(outputs, 0)
    return (features_out, normalize(totals[0]), normalize(totals[1]), normalize(totals[2]), normalize(totals[3]))
```

```python
import functools

import jax
import jax.numpy as jnp
from jax import lax
from jax.experimental import pallas as pl
from jax.experimental.pallas import tpu as pltpu
from jax.sharding import PartitionSpec as P

BLOCK_COUNT = 2
AXES = ("row", "col", "rep")

adapter_scale = 2.0
norm_eps = 1e-06
step_eps = 1e-06
gelu_coef = 0.7978845608
gelu_cubic = 0.044715
F32 = jnp.float32
BF16 = jnp.bfloat16
LANES = 128
SIDE = 8


def padded_2(array, sides, width):
    for axis, dim in sides:
        devices, length = (lax.axis_size(axis), array.shape[dim])
        up = [(i, (i + 1) % devices) for i in range(devices - 1)]
        down = [(j, i) for i, j in up]
        last = lax.slice_in_dim(array, length - width, length, axis=dim)
        first = lax.slice_in_dim(array, 0, width, axis=dim)
        before = lax.ppermute(last, axis, up)
        after = lax.ppermute(first, axis, down)
        array = jnp.concatenate([before, array, after], axis=dim)
    return array


def dot(a, b):
    return lax.dot_general(a, b, (((1,), (0,)), ((), ())), preferred_element_type=F32)


def dot_nt(a, b):
    return lax.dot_general(a, b, (((1,), (1,)), ((), ())), preferred_element_type=F32)


def dot_tn(a, b):
    return lax.dot_general(a, b, (((0,), (0,)), ((), ())), preferred_element_type=F32)


def convolve(x_ref, k_ref, wide, store):
    prows, pcols, chans = x_ref.shape
    rows, cols = prows - 6, pcols - 6

    def chunk(cc, _):
        lanes = pl.ds(pl.multiple_of(cc * LANES, LANES), LANES)

        def widen(r, _):
            wide[r, 0:pcols, :] = x_ref[r, :, lanes].astype(F32)
            return 0

        lax.fori_loop(0, prows, widen, 0)

        def tile(rt, _):
            r0 = rt * SIDE
            for c0 in range(0, cols, SIDE):
                acc = [jnp.zeros((SIDE, LANES), F32) for _ in range(SIDE)]
                for b in range(7):
                    column = [wide[r0 + i, c0 + b : c0 + b + SIDE, :] for i in range(SIDE + 6)]
                    for a in range(7):
                        tap = k_ref[a * 7 + b : a * 7 + b + 1, lanes]
                        for i in range(SIDE):
                            acc[i] = acc[i] + column[i + a] * tap
                for i in range(SIDE):
                    store(r0 + i, c0, lanes, acc[i])
            return 0

        lax.fori_loop(0, rows // SIDE, tile, 0)
        return 0

    lax.fori_loop(0, chans // LANES, chunk, 0)


def conv_norm_kernel(keep, x_ref, k_ref, bias_ref, gain_ref, shift_ref, *refs):
    if keep:
        normed_ref, xhat_ref, rstd_ref, wide, conv = refs
    else:
        normed_ref, wide, conv = refs

    def store(r, c0, lanes, sums):
        conv[r, c0 : c0 + SIDE, lanes] = sums + bias_ref[0:1, lanes]

    convolve(x_ref, k_ref, wide, store)

    def norm(r, _):
        value = conv[r]
        centered = value - jnp.mean(value, -1, keepdims=True)
        rstd = lax.rsqrt(jnp.mean(centered * centered, -1, keepdims=True) + norm_eps)
        xhat = centered * rstd
        normed_ref[r] = (xhat * gain_ref[...] + shift_ref[...]).astype(BF16)
        if keep:
            xhat_ref[r] = xhat.astype(BF16)
            rstd_ref[r] = jnp.broadcast_to(rstd, rstd_ref.shape[1:])
        return 0

    lax.fori_loop(0, conv.shape[0], norm, 0)


def conv_norm(padded, taps, bias, gain, shift, keep):
    prows, pcols, chans = padded.shape
    rows, cols = prows - 6, pcols - 6
    shapes = [jax.ShapeDtypeStruct((rows, cols, chans), BF16)]
    if keep:
        shapes += [
            jax.ShapeDtypeStruct((rows, cols, chans), BF16),
            jax.ShapeDtypeStruct((rows, cols, LANES), F32),
        ]
    return pl.pallas_call(
        functools.partial(conv_norm_kernel, keep),
        out_shape=shapes,
        scratch_shapes=[
            pltpu.VMEM((prows, cols + 8, LANES), F32),
            pltpu.VMEM((rows, cols, chans), F32),
        ],
        name="conv_norm",
    )(padded, taps, bias, gain, shift)


def conv_back_kernel(x_ref, k_ref, cot_ref, scale_ref, out_ref, wide, conv):
    def store(r, c0, lanes, sums):
        conv[r, c0 : c0 + SIDE, lanes] = sums

    convolve(x_ref, k_ref, wide, store)

    def finish(r, _):
        out_ref[r] = ((cot_ref[r].astype(F32) + conv[r]) * scale_ref[...]).astype(BF16)
        return 0

    lax.fori_loop(0, conv.shape[0], finish, 0)


def conv_back(padded, taps, cotangent, scale):
    rows, cols, chans = cotangent.shape
    return pl.pallas_call(
        conv_back_kernel,
        out_shape=jax.ShapeDtypeStruct((rows, cols, chans), BF16),
        scratch_shapes=[
            pltpu.VMEM((rows + 6, cols + 8, LANES), F32),
            pltpu.VMEM((rows, cols, chans), F32),
        ],
        name="conv_back",
    )(padded, taps, cotangent, scale)


def gelu_parts(v, slope):
    square = v * v
    tangent = jnp.tanh(v * (gelu_coef + (gelu_coef * gelu_cubic) * square))
    half = 0.5 * v
    value = half + half * tangent
    if not slope:
        return value, None
    return value, 0.5 * (1.0 + tangent) + half * (1.0 - tangent * tangent) * (
        gelu_coef + (3.0 * gelu_coef * gelu_cubic) * square
    )


def pointwise_kernel(forward, backward, through, *refs):
    refs = list(refs)
    n_ref, w1, wo, a1, b1, ao, bo, scale = refs[:8]
    refs = refs[8:]
    x_ref = refs.pop(0) if forward else None
    g_ref = refs.pop(0) if backward else None
    if through:
        gain, xhat_ref, rstd_ref = refs[:3]
        refs = refs[3:]
    out_ref = refs.pop(0) if forward else None
    gconv_ref = refs.pop(0) if through else None
    grad_ref = refs.pop(0) if backward else None

    pixels, chans = n_ref.shape
    hidden = w1.shape[1]
    piece = min(512, hidden)
    n = n_ref[...]
    mid_in = dot(n, a1[...]).astype(BF16)
    mid_out = jnp.zeros((pixels, a1.shape[1]), F32)
    branch = jnp.zeros((pixels, chans), F32)
    if backward:

        @pl.when(pl.program_id(0) == 0)
        def _():
            grad_ref[...] = jnp.zeros_like(grad_ref)

        go = g_ref[...]
        if forward:
            go = (go.astype(F32) * scale[...]).astype(BF16)
        gm_out = (adapter_scale * dot_nt(go, bo[...])).astype(BF16)
        gm_in = jnp.zeros((pixels, a1.shape[1]), F32)
        gnormed = jnp.zeros((pixels, chans), F32)
    for h in range(0, hidden, piece):
        span = slice(h, h + piece)
        pre = dot(n, w1[:, span]) + adapter_scale * dot(mid_in, b1[:, span])
        value, slope = gelu_parts(pre, backward)
        hid = value.astype(BF16)
        mid_out = mid_out + dot(hid, ao[span, :])
        if forward:
            branch = branch + dot(hid, wo[span, :])
        if backward:
            at = chans + hidden + h
            grad_ref[:, at : at + piece] += dot_tn(gm_out, hid)
            ghid = dot_nt(go, wo[span, :]) + dot_nt(gm_out, ao[span, :])
            gpre = (ghid * slope).astype(BF16)
            at = chans + h
            grad_ref[:, at : at + piece] += adapter_scale * dot_tn(mid_in, gpre)
            gm_in = gm_in + dot_nt(gpre, b1[:, span])
            if through:
                gnormed = gnormed + dot_nt(gpre, w1[:, span])
    mid_out = mid_out.astype(BF16)
    if forward:
        branch = branch + adapter_scale * dot(mid_out, bo[...])
        out_ref[...] = (x_ref[...].astype(F32) + scale[...] * branch).astype(BF16)
    if backward:
        gm_in = (adapter_scale * gm_in).astype(BF16)
        grad_ref[:, :chans] += dot_tn(gm_in, n)
        grad_ref[:, chans + 2 * hidden :] += adapter_scale * dot_tn(mid_out, go)
        if through:
            u = (gnormed + dot_nt(gm_in, a1[...])) * gain[...]
            xhat = xhat_ref[...].astype(F32)
            m1 = jnp.mean(u, -1, keepdims=True)
            m2 = jnp.mean(u * xhat, -1, keepdims=True)
            gconv_ref[...] = (rstd_ref[:, 0:1] * (u - m1 - xhat * m2)).astype(BF16)


def pointwise(layer, normed, weights, scale, x=None, g=None, through=None):
    pixels, chans = normed.shape
    hidden, rank = weights[0].shape[2], weights[2].shape[2]
    tile = min(256, pixels)

    def rows_of(array):
        return pl.BlockSpec((tile, array.shape[1]), lambda i: (i, 0))

    def whole(array):
        return pl.BlockSpec((None,) + array.shape[1:], lambda i: (layer, 0, 0))

    args = [normed, *weights, scale]
    specs = [rows_of(normed)] + [whole(w) for w in weights]
    specs += [pl.BlockSpec((1, chans), lambda i: (0, 0))]
    shapes, outs = [], []
    for array in (x, g):
        if array is not None:
            args.append(array)
            specs.append(rows_of(array))
    if through is not None:
        gain, xhat, rstd = through
        args += [gain, xhat, rstd]
        specs += [pl.BlockSpec((1, chans), lambda i: (0, 0)), rows_of(xhat), rows_of(rstd)]
    count = (x is not None) + (through is not None)
    shapes += [jax.ShapeDtypeStruct((pixels, chans), BF16)] * count
    outs += [rows_of(normed)] * count
    if g is not None:
        width = 2 * (chans + hidden)
        shapes.append(jax.ShapeDtypeStruct((rank, width), F32))
        outs.append(pl.BlockSpec((rank, width), lambda i: (0, 0)))
    return pl.pallas_call(
        functools.partial(pointwise_kernel, x is not None, g is not None, through is not None),
        grid=(pixels // tile,),
        in_specs=specs,
        out_specs=outs,
        out_shape=shapes,
        compiler_params=pltpu.CompilerParams(
            dimension_semantics=("arbitrary",), vmem_limit_bytes=56 * 1024 * 1024
        ),
        name="pointwise",
    )(*args)


def place(index):
    found = {}
    for axis in AXES[::-1]:
        size = lax.axis_size(axis)
        found[axis] = lax.rem(index, size)
        index = lax.div(index, size)
    return found


def reduce_kernel(n, x_ref, out_ref, landed, gathered, s1, r1, s2, r2):
    me = jnp.int32(0)
    for axis in AXES:
        me = me * lax.axis_size(axis) + lax.axis_index(axis)
    barrier = pltpu.get_barrier_semaphore()

    def each(run):
        def step(d, carry):
            run(d, lax.rem(me + d, n))
            return carry

        lax.fori_loop(1, n, step, 0)

    each(
        lambda d, peer: pl.semaphore_signal(
            barrier, inc=1, device_id=place(peer), device_id_type=pl.DeviceIdType.MESH
        )
    )
    pl.semaphore_wait(barrier, n - 1)

    def scatter(d, peer):
        return pltpu.make_async_remote_copy(
            x_ref.at[peer], landed.at[d], s1.at[d], r1.at[d],
            device_id=place(peer), device_id_type=pl.DeviceIdType.MESH,
        )

    def gather(d, peer, slot):
        return pltpu.make_async_remote_copy(
            gathered.at[slot], gathered.at[slot], s2.at[d], r2.at[d],
            device_id=place(peer), device_id_type=pl.DeviceIdType.MESH,
        )

    each(lambda d, peer: scatter(d, peer).start())

    def add(d, total):
        scatter(d, lax.rem(me + d, n)).wait_recv()
        return total + landed[d].astype(F32)

    total = lax.fori_loop(1, n, add, x_ref[me].astype(F32))
    gathered[me] = total.astype(BF16)
    each(lambda d, peer: gather(d, peer, me).start())
    out_ref[me] = gathered[me].astype(F32)

    def take(d, carry):
        slot = lax.rem(me + n - d, n)
        gather(d, slot, slot).wait_recv()
        out_ref[slot] = gathered[slot].astype(F32)
        return carry

    lax.fori_loop(1, n, take, 0)
    each(lambda d, peer: scatter(d, peer).wait_send())
    each(lambda d, peer: gather(d, peer, me).wait_send())


def reduce_all(array):
    n = 1
    for axis in AXES:
        n *= lax.axis_size(axis)
    flat = array.astype(BF16).reshape(-1)
    unit = n * LANES
    pad = -flat.shape[0] % unit
    if pad:
        flat = jnp.pad(flat, (0, pad))
    parts = flat.reshape(n, -1, LANES)
    summed = pl.pallas_call(
        functools.partial(reduce_kernel, n),
        out_shape=jax.ShapeDtypeStruct(parts.shape, F32),
        in_specs=[pl.BlockSpec(memory_space=pltpu.VMEM)],
        out_specs=pl.BlockSpec(memory_space=pltpu.VMEM),
        scratch_shapes=[pltpu.VMEM(parts.shape, BF16)] * 2 + [pltpu.SemaphoreType.DMA((n,))] * 4,
        compiler_params=pltpu.CompilerParams(collective_id=0, has_side_effects=True),
        name="reduce_all",
    )(parts)
    return summed.reshape(-1)[: array.size].reshape(array.shape)


def normalize(stacked):
    mean = jnp.mean(stacked * stacked, axis=(1, 2), keepdims=True)
    return stacked * lax.rsqrt(mean + step_eps)


def body(
    features,
    cotangent,
    depthwise_filters,
    depthwise_bias_vector,
    layernorm_gain,
    layernorm_shift,
    inner_frozen_weight,
    outer_frozen_weight,
    inner_down_factor,
    inner_up_factor,
    outer_down_factor,
    outer_up_factor,
    branch_channel_scale,
):
    images, rows, cols, chans = features.shape
    hidden = inner_frozen_weight.shape[2]
    weights = (
        inner_frozen_weight,
        outer_frozen_weight,
        inner_down_factor,
        inner_up_factor,
        outer_down_factor,
        outer_up_factor,
    )
    sides = (("row", 1), ("col", 2))
    taps = depthwise_filters.reshape(BLOCK_COUNT, 49, chans)
    flip = depthwise_filters[:, ::-1, ::-1, :].reshape(BLOCK_COUNT, 49, chans)

    def flat(a):
        return a.reshape(-1, a.shape[-1])

    def vec(array, layer):
        return array[layer : layer + 1]

    def normed_of(x, layer, keep):
        padded = padded_2(x, sides, 3)
        parts = [
            conv_norm(
                padded[i],
                taps[layer],
                vec(depthwise_bias_vector, layer),
                vec(layernorm_gain, layer),
                vec(layernorm_shift, layer),
                keep,
            )
            for i in range(images)
        ]
        return [flat(jnp.concatenate(p, 0)) if images > 1 else flat(p[0]) for p in zip(*parts)]

    (normed_0,) = normed_of(features, 0, False)
    (x_1,) = pointwise(0, normed_0, weights, vec(branch_channel_scale, 0), x=flat(features))
    normed_1, xhat_1, rstd_1 = normed_of(x_1.reshape(features.shape), 1, True)
    x_2, gconv, grads_1 = pointwise(
        1,
        normed_1,
        weights,
        vec(branch_channel_scale, 1),
        x=x_1,
        g=flat(cotangent),
        through=(vec(layernorm_gain, 1), xhat_1, rstd_1),
    )
    padded = padded_2(gconv.reshape(features.shape), sides, 3)
    go_0 = [
        conv_back(padded[i], flip[1], cotangent[i], vec(branch_channel_scale, 0))
        for i in range(images)
    ]
    go_0 = flat(jnp.concatenate(go_0, 0) if images > 1 else go_0[0])
    (grads_0,) = pointwise(0, normed_0, weights, vec(branch_channel_scale, 0), g=go_0)

    total = reduce_all(jnp.stack([grads_0, grads_1]))
    a_in = total[:, :, :chans].transpose(0, 2, 1)
    b_in = total[:, :, chans : chans + hidden]
    a_out = total[:, :, chans + hidden : chans + 2 * hidden].transpose(0, 2, 1)
    b_out = total[:, :, chans + 2 * hidden :]
    return (
        x_2.reshape(features.shape),
        normalize(a_in),
        normalize(b_in),
        normalize(a_out),
        normalize(b_out),
    )


def solution(mesh):
    pixels = P("rep", "row", "col", None)
    return jax.shard_map(
        body,
        mesh=mesh,
        in_specs=(pixels, pixels) + (P(),) * 11,
        out_specs=(pixels, P(), P(), P(), P()),
        check_vma=False,
    )
```
